32 devices in a mesh: seq: 8 (over z, x), head: 4 (over y, core).
Axes of the slice: x: 2, y: 2, z: 4, core: 2. Of those that a mesh axis runs over, the one named last changes fastest.
Arguments:
- values_in: bfloat16 [4096, 4096], P('seq', 'head'), may hold values from -6 to 6
- gate_in: bfloat16 [4096, 4096], P('seq', 'head'), may hold values from -6 to 6
- key_proj: bfloat16 [4096, 128], P('seq'), may hold values from -0.52734375 to 0.52734375
- query_proj: bfloat16 [4096, 128], P('seq'), may hold values from -6 to 6
- step_size: float32 [4096, 64], P('seq', 'head'), may hold values from 0.5 to 2
- log_decay: float32 [4096, 64], P('seq', 'head'), may hold values from -1.2 to 0
- skip_weight: float32 [64], P('head'), may hold values from 0.5 to 1.5
- norm_gain: float32 [4096], P('head'), may hold values from 0.5 to 1.5
- level_table: float32 [16, 64, 7], P(None, 'head'), may hold values from 0.25 to 2
- level_pick: int32 [4096], P('seq'), may hold values from 0 to 15
- doc_start: int32 [64], P('seq'), may hold values 0 or 1
Outputs:
- layer_out: bfloat16 [4096, 4096], P('seq', 'head')
The draws below stay inside these ranges and needn't reach their ends.
All inputs are finite; a program needn't handle non-finite values. No bound on the sum of `doc_start` on one device may be relied on, other than what follows from the above.
Results may differ from the reference program's by a relative error of at most 0.012.
Values may be sent and summed in bfloat16 or wider, within the bound.
A program may use at most 64 MiB of HBM per device.

```python
import math
import jax
import jax.numpy as jnp
from jax import lax

H = 64
HEADDIM = 64
DSTATE = 128
STRETCH = 64
GROUPS = 16
TOK_DEV = 512
SEQUENCE_TOKENS = 4096
NCHUNK = 64
STRETCH_BITS = 3
SPAN_BITS = 3
LEVELS = 7


def head_rank(key):
    return jax.random.permutation(jax.random.fold_in(key, 101), H)


def class_counts():
    return (max(1, H // 16), max(1, 3 * H // 16), max(1, H // 4))


def draw_log_decay(key, part):
    parallel_sequences = jax.random.split(jax.random.fold_in(key, 7), 8)
    rank = head_rank(key)
    very_count, fast_count, medium_count = class_counts()
    very_rate = jnp.exp(jax.random.uniform(parallel_sequences[0], (H,), minval=math.log(0.5), maxval=math.log(1.0)))
    fast_rate = jnp.exp(jax.random.uniform(parallel_sequences[1], (H,), minval=math.log(0.03), maxval=math.log(0.08)))
    medium_rate = jnp.exp(jax.random.uniform(parallel_sequences[7], (H,), minval=math.log(0.006), maxval=math.log(0.012)))
    slow_rate = jnp.exp(jax.random.uniform(parallel_sequences[2], (H,), minval=math.log(0.03), maxval=math.log(0.3))) * (math.log(10.0) / SEQUENCE_TOKENS)
    head_decay_speed = jnp.where(rank < very_count, very_rate, jnp.where(rank < very_count + fast_count, fast_rate, jnp.where(rank < very_count + fast_count + medium_count, medium_rate, slow_rate)))
    interval_multiplier = jnp.exp(jax.random.uniform(parallel_sequences[3], (SEQUENCE_TOKENS // TOK_DEV, H), minval=-math.log(2.0), maxval=math.log(2.0)))
    interval_multiplier = jnp.repeat(interval_multiplier, TOK_DEV, axis=0)
    noise_multiplier = jnp.exp(jax.random.uniform(parallel_sequences[4], (SEQUENCE_TOKENS, H), minval=-math.log(2.0), maxval=math.log(2.0)))
    outlier_position = jax.random.randint(parallel_sequences[5], (3,), 0, SEQUENCE_TOKENS)
    outlier_length = jax.random.uniform(parallel_sequences[6], (3,), minval=0.22, maxval=0.69)
    element_position = jnp.arange(SEQUENCE_TOKENS, dtype=jnp.int32)
    outlier_penalty = jnp.sum(jnp.where(element_position[:, None] == outlier_position[None, :], outlier_length[None, :], 0.0), axis=1)
    decay_logarithm = -(head_decay_speed[None, :] * interval_multiplier * noise_multiplier) - outlier_penalty[:, None]
    return jnp.maximum(decay_logarithm, -1.2).astype(jnp.float32)


def draw_values_in(key, part):
    parallel_sequences = jax.random.split(jax.random.fold_in(key, 11), 1)
    rank = head_rank(key)
    very_count, fast_count, medium_count = class_counts()
    slow_head = rank >= very_count + fast_count + medium_count
    span_large = jax.random.uniform(jax.random.fold_in(key, 103), (SEQUENCE_TOKENS // TOK_DEV,)) < 0.3
    span_scale = jnp.repeat(jnp.where(span_large, 1.0, 0.02), TOK_DEV)
    head_scale = jnp.where(slow_head[None, :], 2.0 / math.sqrt(SEQUENCE_TOKENS), span_scale[:, None])
    channel_scale = jnp.repeat(head_scale, HEADDIM, axis=1)
    base = jax.random.truncated_normal(parallel_sequences[0], -6.0, 6.0, (SEQUENCE_TOKENS, H * HEADDIM))
    return (base * channel_scale).astype(jnp.bfloat16)


def set_ends(values, key, low, largest):
    index_at = [jax.random.randint(jax.random.fold_in(key, axis), (), 0, length) for axis, length in enumerate(values.shape)]
    longest = values.shape.index(max(values.shape))
    next_to = index_at[:longest] + [(index_at[longest] + 1) % values.shape[longest]] + index_at[longest + 1:]
    return values.at[tuple(index_at)].set(low).at[tuple(next_to)].set(largest)


def levels(key, dims, shards, smallest, top_value):
    factor_of, own = 1.0, jax.random.fold_in(key, 6)
    for dim, blocks in shards:
        steps = jnp.exp(jax.random.uniform(jax.random.fold_in(own, dim), (blocks,), jnp.float32, smallest / len(shards), top_value / len(shards)))
        factor_of = factor_of * jnp.repeat(steps, dims[dim] // blocks).reshape([-1 if axis == dim else 1 for axis in range(len(dims))])
    return factor_of


def noise(stream_key, extent, scale, limit, pieces=(), kind=jnp.bfloat16):
    drawn = scale * jax.random.normal(stream_key, extent, jnp.float32)
    if pieces:
        drawn = drawn * levels(stream_key, extent, pieces, -0.22, 0.18)
    return jnp.clip(drawn, -limit, limit).astype(kind)


def setup_inputs(seed: int = 0) -> dict:
    streams_of = jax.random.split(jax.random.key(seed), 12)
    values_in = draw_values_in(jax.random.fold_in(streams_of[11], 71), 0)
    gate_in = noise(streams_of[1], (SEQUENCE_TOKENS, H * HEADDIM), 1.0, 6.0, ((0, 8), (1, 4)))
    key_proj = noise(streams_of[2], (SEQUENCE_TOKENS, DSTATE), 0.088, 0.52734375, ((0, 8),))
    query_proj = noise(streams_of[3], (SEQUENCE_TOKENS, DSTATE), 1.0, 6.0, ((0, 8),))
    step_size = jnp.clip(jnp.exp(math.log(2.0) - 1.3862944 * jax.random.uniform(streams_of[4], (SEQUENCE_TOKENS, H), jnp.float32) ** levels(streams_of[4], (SEQUENCE_TOKENS, H), ((0, 8), (1, 4)), -0.2, 0.2)), 0.5, 2.0)
    log_decay = draw_log_decay(jax.random.fold_in(streams_of[11], 71), 0)
    skip_weight = jnp.clip(0.5 + 1.0 * jax.random.uniform(streams_of[6], (H,), jnp.float32) ** levels(streams_of[6], (H,), ((0, 4),), -0.2, 0.2), 0.5, 1.5)
    norm_gain = jnp.clip(1.0 + 0.1 * jax.random.normal(streams_of[7], (H * HEADDIM,), jnp.float32), 0.5, 1.5)
    level_table = jnp.clip(jnp.exp(math.log(2.0) - 2.0794415 * jax.random.uniform(streams_of[8], (GROUPS, H, LEVELS), jnp.float32) ** levels(streams_of[8], (GROUPS, H, LEVELS), ((1, 4),), -0.2, 0.2)), 0.25, 2.0)
    level_pick = set_ends(jax.random.randint(streams_of[9], (SEQUENCE_TOKENS,), 0, GROUPS), jax.random.fold_in(streams_of[9], 1), 0, GROUPS - 1).astype(jnp.int32)
    doc_start = set_ends((jax.random.randint(streams_of[10], (NCHUNK,), 0, NCHUNK) < 2).astype(jnp.int32), jax.random.fold_in(streams_of[10], 1), 0, 1)
    return {"values_in": values_in, "gate_in": gate_in, "key_proj": key_proj, "query_proj": query_proj, "step_size": step_size, "log_decay": log_decay, "skip_weight": skip_weight, "norm_gain": norm_gain, "level_table": level_table, "level_pick": level_pick, "doc_start": doc_start}


epsilon = 1e-06

def level_of_pairs(row_count, stretch_len, low_bits):
    blocks = jnp.arange(row_count, dtype=jnp.int32) // stretch_len
    differ = jnp.bitwise_xor(blocks[:, None], blocks[None, :])
    level_index = jnp.zeros((row_count, row_count), jnp.int32)
    for bit_index in range(low_bits):
        level_index = level_index + (differ >= 1 << bit_index).astype(jnp.int32)
    return level_index

def reference(values_in, gate_in, key_proj, query_proj, step_size, log_decay, skip_weight, norm_gain, level_table, level_pick, doc_start):
    span_count = SEQUENCE_TOKENS // TOK_DEV
    per_span = TOK_DEV // STRETCH
    level_index = level_of_pairs(TOK_DEV, STRETCH, STRETCH_BITS)
    element_position = jnp.arange(TOK_DEV, dtype=jnp.int32)
    causal = element_position[:, None] >= element_position[None, :]
    level_weight = level_table[level_pick]
    bit_range = jnp.arange(SPAN_BITS, dtype=jnp.int32)

    def one_span(level_state, inputs):
        span_index, span_values, span_gate, span_keys, span_query, span_step, span_decay_log, span_weight, span_starts = inputs
        log_total = jnp.cumsum(span_decay_log, axis=0)
        doc_stretch = jnp.cumsum(span_starts)
        doc_count = jnp.broadcast_to(doc_stretch[:, None], (per_span, STRETCH)).reshape(TOK_DEV)
        visible = causal & (doc_count[:, None] == doc_count[None, :])
        select = jnp.zeros((H, TOK_DEV, TOK_DEV), jnp.float32)
        for level_id in range(STRETCH_BITS + 1):
            select = select + jnp.where(level_index[None] == level_id, jnp.transpose(span_weight[:, :, level_id])[:, :, None], 0.0)
        total_t = jnp.transpose(log_total)
        log_gap = jnp.where(visible[None], total_t[:, :, None] - total_t[:, None, :], -jnp.inf)
        scores = jnp.dot(span_query, span_keys.T, preferred_element_type=jnp.float32)
        mixing = (scores[None] * select * jnp.exp(log_gap)).astype(jnp.bfloat16)
        scaled_in = (span_step[:, :, None] * span_values.astype(jnp.float32)).astype(jnp.bfloat16)
        local_part = jnp.einsum('hts,shp->thp', mixing.astype(jnp.float32), scaled_in.astype(jnp.float32))
        remote_state = level_state.astype(jnp.bfloat16)
        reach_decay = jnp.exp(log_total) * (doc_count == 0).astype(jnp.float32)[:, None]
        projected = jnp.einsum('tn,bhpn->tbhp', span_query.astype(jnp.float32), remote_state.astype(jnp.float32))
        remote_weight = span_weight[:, :, 1 + STRETCH_BITS:1 + STRETCH_BITS + SPAN_BITS]
        remote_part = reach_decay[:, :, None] * jnp.einsum('thb,tbhp->thp', remote_weight, projected)
        combined = local_part + remote_part + skip_weight[None, :, None] * span_values.astype(jnp.float32)
        gated_out = combined * jax.nn.silu(span_gate.astype(jnp.float32))
        mean_square = lax.optimization_barrier(jnp.mean(gated_out * gated_out, axis=(1, 2), keepdims=True))
        result = (gated_out * lax.rsqrt(mean_square + epsilon) * norm_gain.reshape(H, HEADDIM)[None]).astype(jnp.bfloat16)
        end_log = log_total[TOK_DEV - 1]
        tail_decay = jnp.exp(end_log[None, :] - log_total) * (doc_count == doc_count[TOK_DEV - 1]).astype(jnp.float32)[:, None]
        carried_in = (tail_decay[:, :, None] * scaled_in.astype(jnp.float32)).astype(jnp.bfloat16)
        end_state = jnp.einsum('sn,shp->hpn', span_keys.astype(jnp.float32), carried_in.astype(jnp.float32))
        span_decay = jnp.exp(end_log) * (doc_count[TOK_DEV - 1] == 0).astype(jnp.float32)
        next_index = span_index + 1
        lowest = jnp.bitwise_and(next_index, -next_index)
        target = jnp.sum((jnp.left_shift(jnp.ones_like(bit_range), bit_range) < lowest).astype(jnp.int32))
        below_mask = (bit_range < target).astype(jnp.float32)[:, None, None, None]
        equal_mask = (bit_range == target).astype(jnp.float32)[:, None, None, None]
        above_mask = (bit_range > target).astype(jnp.float32)[:, None, None, None]
        decayed = span_decay[None, :, None, None] * level_state
        merged = lax.optimization_barrier(jnp.sum(below_mask * decayed, axis=0, keepdims=True)) + end_state[None]
        return (above_mask * decayed + equal_mask * merged, result)
    inputs = (jnp.arange(span_count, dtype=jnp.int32), values_in.reshape(span_count, TOK_DEV, H, HEADDIM), gate_in.reshape(span_count, TOK_DEV, H, HEADDIM), key_proj.reshape(span_count, TOK_DEV, DSTATE), query_proj.reshape(span_count, TOK_DEV, DSTATE), step_size.reshape(span_count, TOK_DEV, H), log_decay.reshape(span_count, TOK_DEV, H), level_weight.reshape(span_count, TOK_DEV, H, LEVELS), doc_start.reshape(span_count, per_span))
    start_state = jnp.zeros((SPAN_BITS, H, HEADDIM, DSTATE), jnp.float32)
    final_state, outputs = lax.scan(one_span, start_state, inputs)
    return outputs.reshape(SEQUENCE_TOKENS, H * HEADDIM)
```

```python
import functools

import jax
import jax.numpy as jnp
from jax import lax
from jax.experimental import pallas as pl
from jax.experimental.pallas import tpu as pltpu
from jax.sharding import PartitionSpec as P

HEADDIM = 64
STRETCH = 64
CHUNKS = 4

epsilon = 1e-06
F32 = jnp.float32
BF16 = jnp.bfloat16
MESH = pl.DeviceIdType.MESH


def nt(a, b):
    return lax.dot_general(a, b, (((1,), (1,)), ((), ())), preferred_element_type=F32)


def tn(a, b):
    return lax.dot_general(a, b, (((0,), (0,)), ((), ())), preferred_element_type=F32)


def mm(a, b):
    return jnp.dot(a, b, preferred_element_type=F32)


def split(a):
    high = a.astype(BF16)
    return high, (a - high.astype(F32)).astype(BF16)


def kernel(
    span_bits,
    head_axis,
    doc_ref,
    values_ref,
    gate_ref,
    key_ref,
    query_ref,
    step_ref,
    decay_ref,
    skip_ref,
    gain_ref,
    table_ref,
    pick_ref,
    out_ref,
    total_ref,
    factor_ref,
    score_ref,
    weighted_ref,
    gate_act_ref,
    sum_ref,
    block_ref,
    remote_ref,
    send_ref,
    recv_ref,
    decay_send_ref,
    decay_recv_ref,
    square_send_ref,
    square_recv_ref,
    send_sem,
    recv_sem,
    decay_send_sem,
    decay_recv_sem,
    square_send_sem,
    square_recv_sem,
):
    rows, width = values_ref.shape
    heads = step_ref.shape[1]
    states = key_ref.shape[1]
    stretches = rows // STRETCH
    low_bits = stretches.bit_length() - 1
    table_rows, _, level_count = table_ref.shape
    chunk = width // CHUNKS
    own_seq = lax.axis_index("seq")
    own_head = lax.axis_index("head")

    barrier = pltpu.get_barrier_semaphore()
    for bit in range(span_bits):
        pl.semaphore_signal(
            barrier,
            inc=1,
            device_id={"seq": own_seq ^ (1 << bit), "head": own_head},
            device_id_type=MESH,
        )
    for step in range(1, head_axis):
        pl.semaphore_signal(
            barrier,
            inc=1,
            device_id={"seq": own_seq, "head": lax.rem(own_head + step, head_axis)},
            device_id_type=MESH,
        )

    def state_copy(bit, j):
        return pltpu.make_async_remote_copy(
            src_ref=send_ref.at[bit, j],
            dst_ref=recv_ref.at[bit, j],
            send_sem=send_sem.at[bit, j],
            recv_sem=recv_sem.at[bit, j],
            device_id={"seq": own_seq ^ (1 << bit), "head": own_head},
            device_id_type=MESH,
        )

    def decay_copy(bit):
        return pltpu.make_async_remote_copy(
            src_ref=decay_send_ref.at[bit],
            dst_ref=decay_recv_ref.at[bit],
            send_sem=decay_send_sem.at[bit],
            recv_sem=decay_recv_sem.at[bit],
            device_id={"seq": own_seq ^ (1 << bit), "head": own_head},
            device_id_type=MESH,
        )

    def square_copy(step):
        return pltpu.make_async_remote_copy(
            src_ref=square_send_ref,
            dst_ref=square_recv_ref.at[step - 1],
            send_sem=square_send_sem.at[step - 1],
            recv_sem=square_recv_sem.at[step - 1],
            device_id={"seq": own_seq, "head": lax.rem(own_head + step, head_axis)},
            device_id_type=MESH,
        )

    row_id = lax.broadcasted_iota(jnp.int32, (rows, rows), 0)
    col_id = lax.broadcasted_iota(jnp.int32, (rows, rows), 1)
    lower = (row_id >= col_id).astype(F32).astype(BF16)
    log_decay = decay_ref[...]
    high, rest = split(log_decay)
    middle, low = split(log_decay - high.astype(F32))
    total = mm(lower, high) + (mm(lower, middle) + mm(lower, low))
    total_ref[...] = total
    end_log = total_ref[rows - 1 : rows, :]

    counts = []
    running = doc_ref[0]
    for c in range(stretches):
        if c:
            running = running + doc_ref[c]
        counts.append(running)

    def same(a, b):
        return (a == b).astype(F32)

    for c in range(stretches):
        here = slice(c * STRETCH, (c + 1) * STRETCH)
        factor_ref[0, here, :] = (
            jnp.exp(end_log - total_ref[here, :]) * step_ref[here, :] * same(counts[c], counts[-1])
        ).astype(BF16)

    head_row = lax.broadcasted_iota(jnp.int32, (heads, chunk), 0)
    head_lane = lax.broadcasted_iota(jnp.int32, (heads, chunk), 1) // HEADDIM

    def spread(j):
        return (head_row == head_lane + j * (chunk // HEADDIM)).astype(F32).astype(BF16)

    whole_row = lax.broadcasted_iota(jnp.int32, (heads, width), 0)
    whole_lane = lax.broadcasted_iota(jnp.int32, (heads, width), 1) // HEADDIM
    whole_spread = (whole_row == whole_lane).astype(F32).astype(BF16)

    def widen(row):
        a = jnp.broadcast_to(row, (16, heads))
        first, second = split(a)
        second, third = split(a - first.astype(F32))
        whole = mm(first, whole_spread) + (mm(second, whole_spread) + mm(third, whole_spread))
        return whole[0:1, :]

    span_decay = widen(jnp.exp(end_log)) * same(counts[-1], 0)
    decay_send_ref[0] = span_decay

    for j in range(CHUNKS):
        lanes = slice(j * chunk, (j + 1) * chunk)
        carried = (mm(factor_ref[0], spread(j)) * values_ref[:, lanes].astype(F32)).astype(BF16)
        state = tn(key_ref[...], carried)
        block_ref[j] = state
        send_ref[0, j] = state.astype(BF16)
        if j == 0:
            pl.semaphore_wait(barrier, span_bits + head_axis - 1)
            decay_copy(0).start()
        state_copy(0, j).start()

    part_row = lax.broadcasted_iota(jnp.int32, (table_rows * heads, level_count * heads), 0)
    part_lane = lax.broadcasted_iota(jnp.int32, (table_rows * heads, level_count * heads), 1)
    level_row = lax.broadcasted_iota(jnp.int32, (level_count, level_count * heads), 0)
    level_lane = lax.broadcasted_iota(jnp.int32, (level_count, level_count * heads), 1) // heads
    to_level = (level_row == level_lane).astype(F32).astype(BF16)
    table = table_ref[...].reshape(table_rows * heads, level_count)
    own = part_row % heads == part_lane % heads
    table_high, table_low = split(table)
    picked = (
        lax.broadcasted_iota(jnp.int32, (table_rows * heads, rows), 0) // heads == pick_ref[...]
    )
    picked = picked.astype(F32).astype(BF16)
    level_weight = tn(picked, jnp.where(own, mm(table_high, to_level), 0.0).astype(BF16)) + tn(
        picked, jnp.where(own, mm(table_low, to_level), 0.0).astype(BF16)
    )

    def weight(c, level):
        return level_weight[c * STRETCH : (c + 1) * STRETCH, level * heads : (level + 1) * heads]

    for c in range(stretches):
        here = slice(c * STRETCH, (c + 1) * STRETCH)
        log_here = total_ref[here, :]
        step_here = step_ref[here, :]
        middle_at = c * STRETCH + STRETCH // 2
        offset = log_here - total_ref[middle_at : middle_at + 1, :]
        factor_ref[1, here, :] = (jnp.exp(-offset) * step_here).astype(BF16)
        factor_ref[2, here, :] = (jnp.exp(offset) * weight(c, 0)).astype(BF16)
        for level in range(1, low_bits + 1):
            last = ((c >> level) << level) + (1 << (level - 1)) - 1
            edge = (last + 1) * STRETCH - 1
            keep = same(counts[c], counts[last])
            offset = log_here - total_ref[edge : edge + 1, :]
            if c >> (level - 1) & 1:
                value = jnp.exp(offset) * (weight(c, level) * keep)
            else:
                value = jnp.exp(-offset) * (step_here * keep)
            factor_ref[2 + level, here, :] = value.astype(BF16)
        reach = jnp.exp(log_here) * same(counts[c], 0)
        for bit in range(span_bits):
            upper = lax.rem(own_seq >> bit, 2).astype(F32)
            factor_ref[3 + low_bits + bit, here, :] = (
                reach * weight(c, 1 + low_bits + bit) * upper
            ).astype(BF16)

    tri_row = lax.broadcasted_iota(jnp.int32, (STRETCH, STRETCH), 0)
    tri_col = lax.broadcasted_iota(jnp.int32, (STRETCH, STRETCH), 1)
    for c in range(stretches):
        here = slice(c * STRETCH, (c + 1) * STRETCH)
        line = nt(query_ref[here, :], key_ref[0 : (c + 1) * STRETCH, :])
        if c:
            score_ref[here, 0 : c * STRETCH] = line[:, 0 : c * STRETCH].astype(BF16)
        score_ref[here, here] = jnp.where(tri_row >= tri_col, line[:, here], 0.0).astype(BF16)

    skip = widen(skip_ref[...])

    for j in range(CHUNKS):
        lanes = slice(j * chunk, (j + 1) * chunk)
        to_lanes = spread(j)
        values = values_ref[:, lanes].astype(F32)
        weighted_ref[...] = (mm(factor_ref[1], to_lanes) * values).astype(BF16)
        scale = mm(factor_ref[2], to_lanes)
        base = skip[:, lanes] * values
        for c in range(stretches):
            here = slice(c * STRETCH, (c + 1) * STRETCH)
            sum_ref[j, here, :] = base[here, :] + scale[here, :] * mm(
                score_ref[here, here], weighted_ref[here, :]
            )
        for level in range(1, low_bits + 1):
            half = STRETCH << (level - 1)
            scale = mm(factor_ref[2 + level], to_lanes)
            for start in range(0, rows, 2 * half):
                before = slice(start, start + half)
                after = slice(start + half, start + 2 * half)
                weighted = (scale[before, :] * values[before, :]).astype(BF16)
                sum_ref[j, after, :] += scale[after, :] * mm(score_ref[after, before], weighted)
        gate = gate_ref[:, lanes].astype(F32)
        gate_act_ref[j] = gate * (0.5 + 0.5 * jnp.tanh(0.5 * gate))

    def add_remote(bit, j):
        sum_ref[j] += mm(factor_ref[3 + low_bits + bit], spread(j)) * mm(
            query_ref[...], remote_ref[bit, j]
        )

    block_decay = span_decay
    lead_decay = jnp.ones_like(span_decay)
    for bit in range(span_bits):
        upper = lax.rem(own_seq >> bit, 2).astype(F32)
        decay_copy(bit).wait()
        other_decay = decay_recv_ref[bit]
        keep_own = upper + (1.0 - upper) * other_decay
        keep_other = upper * block_decay + (1.0 - upper)
        next_decay = block_decay * other_decay
        if bit + 1 < span_bits:
            decay_send_ref[bit + 1] = next_decay
            decay_copy(bit + 1).start()
        for j in range(CHUNKS):
            lanes = slice(j * chunk, (j + 1) * chunk)
            state_copy(bit, j).wait()
            other = recv_ref[bit, j].astype(F32)
            if bit + 1 < span_bits:
                merged = keep_own[:, lanes] * block_ref[j] + keep_other[:, lanes] * other
                block_ref[j] = merged
                send_ref[bit + 1, j] = merged.astype(BF16)
                state_copy(bit + 1, j).start()
            remote_ref[bit, j] = (lead_decay[:, lanes] * other).astype(BF16)
            if bit + 1 == span_bits:
                add_remote(bit, j)
        if bit + 1 < span_bits:
            for j in range(CHUNKS):
                add_remote(bit, j)
        lead_decay = lead_decay * (upper * other_decay + (1.0 - upper))
        block_decay = next_decay

    squares = jnp.zeros((rows, chunk), F32)
    for j in range(CHUNKS):
        gated = sum_ref[j] * gate_act_ref[j]
        sum_ref[j] = gated
        squares = squares + gated * gated
    ones = jnp.ones((16, chunk), BF16)
    square_high, square_low = split(squares)
    square_row = nt(ones, square_high) + nt(ones, square_low)
    square_send_ref[...] = square_row[0:1, :]
    for step in range(1, head_axis):
        square_copy(step).start()
    square_total = square_row[0:1, :]
    for step in range(1, head_axis):
        square_copy(step).wait()
        square_total = square_total + square_recv_ref[step - 1]
    mean_square = square_total * (1.0 / (width * head_axis))
    inverse = lax.rsqrt(mean_square + epsilon)
    inverse = jnp.broadcast_to(inverse, (8, rows)).T[:, 0:1]
    for j in range(CHUNKS):
        lanes = slice(j * chunk, (j + 1) * chunk)
        out_ref[:, lanes] = (sum_ref[j] * inverse * gain_ref[:, lanes]).astype(BF16)


def local(
    span_bits,
    head_axis,
    values_in,
    gate_in,
    key_proj,
    query_proj,
    step_size,
    log_decay,
    skip_weight,
    norm_gain,
    level_table,
    level_pick,
    doc_start,
):
    rows, width = values_in.shape
    heads = step_size.shape[1]
    states = key_proj.shape[1]
    low_bits = (rows // STRETCH).bit_length() - 1
    chunk = width // CHUNKS
    vmem = pl.BlockSpec(memory_space=pltpu.VMEM)
    bits = max(span_bits, 1)
    peers = max(head_axis - 1, 1)
    return pl.pallas_call(
        functools.partial(kernel, span_bits, head_axis),
        out_shape=jax.ShapeDtypeStruct((rows, width), BF16),
        in_specs=[pl.BlockSpec(memory_space=pltpu.SMEM)] + [vmem] * 10,
        out_specs=vmem,
        scratch_shapes=[
            pltpu.VMEM((rows, heads), F32),
            pltpu.VMEM((3 + low_bits + span_bits, rows, heads), BF16),
            pltpu.VMEM((rows, rows), BF16),
            pltpu.VMEM((rows, chunk), BF16),
            pltpu.VMEM((CHUNKS, rows, chunk), F32),
            pltpu.VMEM((CHUNKS, rows, chunk), F32),
            pltpu.VMEM((CHUNKS, states, chunk), F32),
            pltpu.VMEM((bits, CHUNKS, states, chunk), BF16),
            pltpu.VMEM((bits, CHUNKS, states, chunk), BF16),
            pltpu.VMEM((bits, CHUNKS, states, chunk), BF16),
            pltpu.VMEM((bits, 1, width), F32),
            pltpu.VMEM((bits, 1, width), F32),
            pltpu.VMEM((1, rows), F32),
            pltpu.VMEM((peers, 1, rows), F32),
            pltpu.SemaphoreType.DMA((bits, CHUNKS)),
            pltpu.SemaphoreType.DMA((bits, CHUNKS)),
            pltpu.SemaphoreType.DMA((bits,)),
            pltpu.SemaphoreType.DMA((bits,)),
            pltpu.SemaphoreType.DMA((peers,)),
            pltpu.SemaphoreType.DMA((peers,)),
        ],
        compiler_params=pltpu.CompilerParams(
            collective_id=0, has_side_effects=True, vmem_limit_bytes=48 * 1024 * 1024
        ),
    )(
        doc_start,
        values_in,
        gate_in,
        key_proj,
        query_proj,
        step_size,
        log_decay,
        skip_weight.reshape(1, heads),
        norm_gain.reshape(1, width),
        level_table,
        level_pick.reshape(1, rows),
    )


def solution(mesh):
    in_specs = (
        P("seq", "head"),
        P("seq", "head"),
        P("seq", None),
        P("seq", None),
        P("seq", "head"),
        P("seq", "head"),
        P("head"),
        P("head"),
        P(None, "head", None),
        P("seq"),
        P("seq"),
    )
    span_bits = mesh.shape["seq"].bit_length() - 1
    body = functools.partial(local, span_bits, mesh.shape["head"])
    return jax.shard_map(
        body, mesh=mesh, in_specs=in_specs, out_specs=P("seq", "head"), check_vma=False
    )
```

```python
import functools

import jax
import jax.numpy as jnp
from jax import lax
from jax.experimental import pallas as pl
from jax.experimental.pallas import tpu as pltpu
from jax.sharding import PartitionSpec as P

HEADDIM = 64
STRETCH = 64
CHUNKS = 4

epsilon = 1e-06
F32 = jnp.float32
BF16 = jnp.bfloat16
MESH = pl.DeviceIdType.MESH


def nt(a, b):
    return lax.dot_general(a, b, (((1,), (1,)), ((), ())), preferred_element_type=F32)


def tn(a, b):
    return lax.dot_general(a, b, (((0,), (0,)), ((), ())), preferred_element_type=F32)


def mm(a, b):
    return jnp.dot(a, b, preferred_element_type=F32)


def split(a):
    high = a.astype(BF16)
    return high, (a - high.astype(F32)).astype(BF16)


def kernel(
    span_bits,
    head_axis,
    values_hbm,
    gate_hbm,
    key_hbm,
    query_hbm,
    step_hbm,
    decay_hbm,
    skip_hbm,
    gain_hbm,
    table_hbm,
    pick_hbm,
    doc_hbm,
    out_ref,
    values_ref,
    gate_ref,
    key_ref,
    query_ref,
    step_ref,
    decay_ref,
    skip_ref,
    gain_ref,
    table_ref,
    pick_ref,
    doc_ref,
    order_ref,
    end_factor_ref,
    factor_ref,
    score_ref,
    weighted_ref,
    gate_act_ref,
    sum_ref,
    block_ref,
    remote_ref,
    send_ref,
    recv_ref,
    decay_send_ref,
    decay_recv_ref,
    square_send_ref,
    square_recv_ref,
    load_sem,
    send_sem,
    recv_sem,
    decay_send_sem,
    decay_recv_sem,
    square_send_sem,
    square_recv_sem,
):
    rows, width = values_ref.shape
    heads = step_ref.shape[0]
    states = key_ref.shape[1]
    stretches = rows // STRETCH
    low_bits = stretches.bit_length() - 1
    level_count, table_rows, _ = table_ref.shape
    chunk = width // CHUNKS
    own_seq = lax.axis_index("seq")
    own_head = lax.axis_index("head")

    pairs = [
        (decay_hbm, decay_ref),
        (doc_hbm, doc_ref),
        (step_hbm, step_ref),
        (key_hbm, key_ref),
        (values_hbm, values_ref),
        (query_hbm, query_ref),
        (pick_hbm, pick_ref),
        (table_hbm, table_ref),
        (skip_hbm, skip_ref),
        (gain_hbm, gain_ref),
        (gate_hbm, gate_ref),
    ]
    loads = [
        pltpu.make_async_copy(source, target, load_sem.at[i])
        for i, (source, target) in enumerate(pairs)
    ]
    for load in loads:
        load.start()

    barrier = pltpu.get_barrier_semaphore()
    for bit in range(span_bits):
        pl.semaphore_signal(
            barrier,
            inc=1,
            device_id={"seq": own_seq ^ (1 << bit), "head": own_head},
            device_id_type=MESH,
        )
    for step in range(1, head_axis):
        pl.semaphore_signal(
            barrier,
            inc=1,
            device_id={"seq": own_seq, "head": lax.rem(own_head + step, head_axis)},
            device_id_type=MESH,
        )

    def state_copy(bit, j):
        return pltpu.make_async_remote_copy(
            src_ref=send_ref.at[bit, j],
            dst_ref=recv_ref.at[bit, j],
            send_sem=send_sem.at[bit, j],
            recv_sem=recv_sem.at[bit, j],
            device_id={"seq": own_seq ^ (1 << bit), "head": own_head},
            device_id_type=MESH,
        )

    def decay_copy(bit):
        return pltpu.make_async_remote_copy(
            src_ref=decay_send_ref.at[bit],
            dst_ref=decay_recv_ref.at[bit],
            send_sem=decay_send_sem.at[bit],
            recv_sem=decay_recv_sem.at[bit],
            device_id={"seq": own_seq ^ (1 << bit), "head": own_head},
            device_id_type=MESH,
        )

    def square_copy(step):
        return pltpu.make_async_remote_copy(
            src_ref=square_send_ref,
            dst_ref=square_recv_ref.at[step - 1],
            send_sem=square_send_sem.at[step - 1],
            recv_sem=square_recv_sem.at[step - 1],
            device_id={"seq": own_seq, "head": lax.rem(own_head + step, head_axis)},
            device_id_type=MESH,
        )

    row_id = lax.broadcasted_iota(jnp.int32, (rows, rows), 0)
    col_id = lax.broadcasted_iota(jnp.int32, (rows, rows), 1)
    order_ref[...] = (row_id <= col_id).astype(F32).astype(BF16)
    whole_row = lax.broadcasted_iota(jnp.int32, (heads, width), 0)
    whole_lane = lax.broadcasted_iota(jnp.int32, (heads, width), 1) // HEADDIM
    whole_spread = (whole_row == whole_lane).astype(F32).astype(BF16)
    lane = lax.broadcasted_iota(jnp.int32, (heads, rows), 1)

    loads[0].wait()
    loads[1].wait()
    log_decay = decay_ref[...]
    high, rest = split(log_decay)
    middle, low = split(log_decay - high.astype(F32))
    total = mm(jnp.concatenate([high, middle, low], axis=0), order_ref[...])
    total = total[0:heads] + (total[heads : 2 * heads] + total[2 * heads : 3 * heads])
    doc_row = lax.broadcasted_iota(jnp.int32, (stretches, rows), 0)
    doc_lane = lax.broadcasted_iota(jnp.int32, (stretches, rows), 1) // STRETCH
    doc_order = (doc_row <= doc_lane).astype(F32).astype(BF16)
    doc = jnp.broadcast_to(doc_ref[...].astype(F32), (16, stretches)).astype(BF16)
    count = mm(doc, doc_order)
    if heads != 16:
        count = jnp.broadcast_to(count[0:1], (heads, rows))

    def at_edges(array, size, edge):
        pieces = []
        for start in range(0, rows, max(size, 128)):
            piece = jnp.broadcast_to(
                array[:, start + edge : start + edge + 1], (heads, max(size, 128))
            )
            if size < 128:
                other = jnp.broadcast_to(
                    array[:, start + size + edge : start + size + edge + 1], (heads, 128)
                )
                piece = jnp.where(lane[:, 0:128] < size, piece, other)
            pieces.append(piece)
        return jnp.concatenate(pieces, axis=1) if len(pieces) > 1 else pieces[0]

    end_log = total[:, rows - 1 : rows]
    end_count = count[:, rows - 1 : rows]
    same_end = (count == end_count).astype(F32)
    loads[2].wait()
    step = step_ref[...]
    end_factor = jnp.exp(end_log - total) * step * same_end
    end_factor_ref[...] = end_factor.T.astype(BF16)

    def widen(column):
        a = jnp.broadcast_to(column, (heads, 128)).T[0:16, :]
        first, rest = split(a)
        second, third = split(rest32(a, first))
        stacked = jnp.concatenate([first, second, third], axis=0)
        whole = mm(stacked, whole_spread)
        return whole[0:1] + (whole[16:17] + whole[32:33])

    def rest32(a, first):
        return a - first.astype(F32)

    span_decay = widen(jnp.exp(end_log) * (end_count == 0.0).astype(F32))
    decay_send_ref[0] = span_decay

    loads[3].wait()
    loads[4].wait()
    for j in range(CHUNKS):
        lanes = slice(j * chunk, (j + 1) * chunk)
        carried = (
            mm(end_factor_ref[...], whole_spread[:, lanes]) * values_ref[:, lanes].astype(F32)
        ).astype(BF16)
        state = tn(key_ref[...], carried)
        block_ref[j] = state
        send_ref[0, j] = state.astype(BF16)
        if j == 0:
            pl.semaphore_wait(barrier, span_bits + head_axis - 1)
            decay_copy(0).start()
        state_copy(0, j).start()

    for load in loads[5:]:
        load.wait()
    picked = (
        lax.broadcasted_iota(jnp.int32, (table_rows, rows), 0) == pick_ref[...]
    )
    picked = picked.astype(F32).astype(BF16)

    def weight(level):
        table_high, table_low = split(table_ref[level])
        return tn(table_high, picked) + tn(table_low, picked)

    factors = []
    offset = total - at_edges(total, STRETCH, STRETCH // 2)
    factors.append(jnp.exp(-offset) * step)
    factors.append(jnp.exp(offset) * weight(0))
    for level in range(1, low_bits + 1):
        size = STRETCH << level
        offset = total - at_edges(total, size, size // 2 - 1)
        keep = (count == at_edges(count, size, size // 2 - 1)).astype(F32)
        after = lane % size >= size // 2
        decayed = jnp.exp(jnp.minimum(jnp.where(after, offset, -offset), 0.0))
        factors.append(decayed * keep * jnp.where(after, weight(level), step))
    reach = jnp.exp(total) * (count == 0.0).astype(F32)
    for bit in range(span_bits):
        upper = lax.rem(own_seq >> bit, 2).astype(F32)
        factors.append(reach * weight(1 + low_bits + bit) * upper)
    per_group = 128 // heads
    for group in range(factor_ref.shape[0]):
        part = factors[group * per_group : (group + 1) * per_group]
        part = part + [jnp.zeros((heads, rows), F32)] * (per_group - len(part))
        factor_ref[group] = jnp.concatenate(part, axis=0).T.astype(BF16)

    spread_row = lax.broadcasted_iota(jnp.int32, (128, chunk), 0)
    spread_lane = lax.broadcasted_iota(jnp.int32, (128, chunk), 1) // HEADDIM

    def spread(k, j):
        first = (k % per_group) * heads + j * (chunk // HEADDIM)
        pick = (spread_row == spread_lane + first).astype(F32).astype(BF16)
        return mm(factor_ref[k // per_group], pick)

    tri_row = lax.broadcasted_iota(jnp.int32, (STRETCH, STRETCH), 0)
    tri_col = lax.broadcasted_iota(jnp.int32, (STRETCH, STRETCH), 1)
    for c in range(stretches):
        here = slice(c * STRETCH, (c + 1) * STRETCH)
        line = nt(query_ref[here, :], key_ref[0 : (c + 1) * STRETCH, :])
        if c:
            score_ref[here, 0 : c * STRETCH] = line[:, 0 : c * STRETCH].astype(BF16)
        score_ref[here, here] = jnp.where(tri_row >= tri_col, line[:, here], 0.0).astype(BF16)

    skip_high, skip_rest = split(jnp.broadcast_to(skip_ref[...], (16, heads)))
    skip_low = (skip_ref[...] - skip_high[0:1].astype(F32)).astype(BF16)
    skip = mm(skip_high, whole_spread) + mm(jnp.broadcast_to(skip_low, (16, heads)), whole_spread)
    skip = skip[0:1, :]

    def local_part(j):
        lanes = slice(j * chunk, (j + 1) * chunk)
        values = values_ref[:, lanes].astype(F32)
        weighted_ref[...] = (spread(0, j) * values).astype(BF16)
        scale = spread(1, j)
        base = skip[:, lanes] * values
        for c in range(stretches):
            here = slice(c * STRETCH, (c + 1) * STRETCH)
            sum_ref[j, here, :] = base[here, :] + scale[here, :] * mm(
                score_ref[here, here], weighted_ref[here, :]
            )
        for level in range(1, low_bits + 1):
            half = STRETCH << (level - 1)
            scale = spread(1 + level, j)
            for start in range(0, rows, 2 * half):
                before = slice(start, start + half)
                after = slice(start + half, start + 2 * half)
                weighted = (scale[before, :] * values[before, :]).astype(BF16)
                sum_ref[j, after, :] += scale[after, :] * mm(score_ref[after, before], weighted)
        gate = gate_ref[:, lanes].astype(F32)
        gate_act_ref[j] = gate * (0.5 + 0.5 * jnp.tanh(0.5 * gate))

    for j in range(CHUNKS):
        local_part(j)

    def add_remote(bit, j):
        sum_ref[j] += spread(2 + low_bits + bit, j) * mm(query_ref[...], remote_ref[bit, j])

    block_decay = span_decay
    lead_decay = jnp.ones_like(span_decay)
    for bit in range(span_bits):
        upper = lax.rem(own_seq >> bit, 2).astype(F32)
        decay_copy(bit).wait()
        other_decay = decay_recv_ref[bit]
        keep_own = upper + (1.0 - upper) * other_decay
        keep_other = upper * block_decay + (1.0 - upper)
        next_decay = block_decay * other_decay
        if bit + 1 < span_bits:
            decay_send_ref[bit + 1] = next_decay
            decay_copy(bit + 1).start()
        for j in range(CHUNKS):
            lanes = slice(j * chunk, (j + 1) * chunk)
            state_copy(bit, j).wait()
            other = recv_ref[bit, j].astype(F32)
            if bit + 1 < span_bits:
                merged = keep_own[:, lanes] * block_ref[j] + keep_other[:, lanes] * other
                block_ref[j] = merged
                send_ref[bit + 1, j] = merged.astype(BF16)
                state_copy(bit + 1, j).start()
            remote_ref[bit, j] = (lead_decay[:, lanes] * other).astype(BF16)
            if bit + 1 == span_bits:
                add_remote(bit, j)
        if bit + 1 < span_bits:
            for j in range(CHUNKS):
                add_remote(bit, j)
        lead_decay = lead_decay * (upper * other_decay + (1.0 - upper))
        block_decay = next_decay

    squares = jnp.zeros((rows, chunk), F32)
    for j in range(CHUNKS):
        gated = sum_ref[j] * gate_act_ref[j]
        sum_ref[j] = gated
        squares = squares + gated * gated
    ones = jnp.ones((16, chunk), BF16)
    square_high, square_low = split(squares)
    square_row = nt(ones, square_high) + nt(ones, square_low)
    square_send_ref[...] = square_row[0:1, :]
    for step in range(1, head_axis):
        square_copy(step).start()
    square_total = square_row[0:1, :]
    for step in range(1, head_axis):
        square_copy(step).wait()
        square_total = square_total + square_recv_ref[step - 1]
    mean_square = square_total * (1.0 / (width * head_axis))
    inverse = lax.rsqrt(mean_square + epsilon)
    inverse = jnp.broadcast_to(inverse, (8, rows)).T[:, 0:1]
    for j in range(CHUNKS):
        lanes = slice(j * chunk, (j + 1) * chunk)
        out_ref[:, lanes] = (sum_ref[j] * inverse * gain_ref[:, lanes]).astype(BF16)


def local(
    span_bits,
    head_axis,
    values_in,
    gate_in,
    key_proj,
    query_proj,
    step_size,
    log_decay,
    skip_weight,
    norm_gain,
    level_table,
    level_pick,
    doc_start,
):
    rows, width = values_in.shape
    heads = step_size.shape[1]
    states = key_proj.shape[1]
    low_bits = (rows // STRETCH).bit_length() - 1
    chunk = width // CHUNKS
    hbm = pl.BlockSpec(memory_space=pltpu.HBM)
    bits = max(span_bits, 1)
    peers = max(head_axis - 1, 1)
    factor_count = 2 + low_bits + span_bits
    groups = -(-factor_count // (128 // heads))
    operands = (
        values_in,
        gate_in,
        key_proj,
        query_proj,
        step_size.T,
        log_decay.T,
        skip_weight.reshape(1, heads),
        norm_gain.reshape(1, width),
        level_table.transpose(2, 0, 1),
        level_pick.reshape(1, rows),
        doc_start.reshape(1, rows // STRETCH),
    )
    return pl.pallas_call(
        functools.partial(kernel, span_bits, head_axis),
        out_shape=jax.ShapeDtypeStruct((rows, width), BF16),
        in_specs=[hbm] * len(operands),
        out_specs=pl.BlockSpec(memory_space=pltpu.VMEM),
        scratch_shapes=[pltpu.VMEM(a.shape, a.dtype) for a in operands]
        + [
            pltpu.VMEM((rows, rows), BF16),
            pltpu.VMEM((rows, heads), BF16),
            pltpu.VMEM((groups, rows, 128), BF16),
            pltpu.VMEM((rows, rows), BF16),
            pltpu.VMEM((rows, chunk), BF16),
            pltpu.VMEM((CHUNKS, rows, chunk), F32),
            pltpu.VMEM((CHUNKS, rows, chunk), F32),
            pltpu.VMEM((CHUNKS, states, chunk), F32),
            pltpu.VMEM((bits, CHUNKS, states, chunk), BF16),
            pltpu.VMEM((bits, CHUNKS, states, chunk), BF16),
            pltpu.VMEM((bits, CHUNKS, states, chunk), BF16),
            pltpu.VMEM((bits, 1, width), F32),
            pltpu.VMEM((bits, 1, width), F32),
            pltpu.VMEM((1, rows), F32),
            pltpu.VMEM((peers, 1, rows), F32),
            pltpu.SemaphoreType.DMA((len(operands),)),
            pltpu.SemaphoreType.DMA((bits, CHUNKS)),
            pltpu.SemaphoreType.DMA((bits, CHUNKS)),
            pltpu.SemaphoreType.DMA((bits,)),
            pltpu.SemaphoreType.DMA((bits,)),
            pltpu.SemaphoreType.DMA((peers,)),
            pltpu.SemaphoreType.DMA((peers,)),
        ],
        compiler_params=pltpu.CompilerParams(
            collective_id=0, has_side_effects=True, vmem_limit_bytes=60 * 1024 * 1024
        ),
    )(*operands)


def solution(mesh):
    in_specs = (
        P("seq", "head"),
        P("seq", "head"),
        P("seq", None),
        P("seq", None),
        P("seq", "head"),
        P("seq", "head"),
        P("head"),
        P("head"),
        P(None, "head", None),
        P("seq"),
        P("seq"),
    )
    span_bits = mesh.shape["seq"].bit_length() - 1
    body = functools.partial(local, span_bits, mesh.shape["head"])
    return jax.shard_map(
        body, mesh=mesh, in_specs=in_specs, out_specs=P("seq", "head"), check_vma=False
    )
```

```python
import functools

import jax
import jax.numpy as jnp
from jax import lax
from jax.experimental import pallas as pl
from jax.experimental.pallas import tpu as pltpu
from jax.sharding import PartitionSpec as P

HEADDIM = 64
STRETCH = 64
CHUNKS = 4

epsilon = 1e-06
F32 = jnp.float32
BF16 = jnp.bfloat16
MESH = pl.DeviceIdType.MESH


def nt(a, b):
    return lax.dot_general(a, b, (((1,), (1,)), ((), ())), preferred_element_type=F32)


def tn(a, b):
    return lax.dot_general(a, b, (((0,), (0,)), ((), ())), preferred_element_type=F32)


def mm(a, b):
    return jnp.dot(a, b, preferred_element_type=F32)


def split(a):
    high = a.astype(BF16)
    return high, (a - high.astype(F32)).astype(BF16)


def kernel(
    span_bits,
    head_axis,
    values_hbm,
    gate_hbm,
    key_hbm,
    query_hbm,
    step_hbm,
    decay_hbm,
    skip_hbm,
    gain_hbm,
    table_hbm,
    pick_hbm,
    doc_hbm,
    out_ref,
    values_ref,
    gate_ref,
    key_ref,
    query_ref,
    step_ref,
    decay_ref,
    skip_ref,
    gain_ref,
    table_ref,
    pick_ref,
    doc_ref,
    order_ref,
    end_factor_ref,
    factor_ref,
    score_ref,
    weighted_ref,
    gate_act_ref,
    sum_ref,
    block_ref,
    remote_ref,
    send_ref,
    recv_ref,
    decay_send_ref,
    decay_recv_ref,
    square_send_ref,
    square_recv_ref,
    row_ref,
    square_ref,
    load_sem,
    send_sem,
    recv_sem,
    decay_send_sem,
    decay_recv_sem,
    square_send_sem,
    square_recv_sem,
    forward_sem,
):
    rows, width = values_ref.shape
    heads = step_ref.shape[0]
    states = key_ref.shape[1]
    stretches = rows // STRETCH
    low_bits = stretches.bit_length() - 1
    level_count, table_rows, _ = table_ref.shape
    chunk = width // CHUNKS
    own_seq = lax.axis_index("seq")
    own_head = lax.axis_index("head")

    pairs = [
        (decay_hbm, decay_ref),
        (doc_hbm, doc_ref),
        (step_hbm, step_ref),
        (key_hbm, key_ref),
        (values_hbm, values_ref),
        (query_hbm, query_ref),
        (pick_hbm, pick_ref),
        (table_hbm, table_ref),
        (skip_hbm, skip_ref),
        (gain_hbm, gain_ref),
        (gate_hbm, gate_ref),
    ]
    loads = [
        pltpu.make_async_copy(source, target, load_sem.at[i])
        for i, (source, target) in enumerate(pairs)
    ]
    for load in loads:
        load.start()

    barrier = pltpu.get_barrier_semaphore()
    for bit in range(span_bits):
        pl.semaphore_signal(
            barrier,
            inc=1,
            device_id={"seq": own_seq ^ (1 << bit), "head": own_head},
            device_id_type=MESH,
        )
    for step in range(1, head_axis):
        pl.semaphore_signal(
            barrier,
            inc=1,
            device_id={"seq": own_seq, "head": lax.rem(own_head + step, head_axis)},
            device_id_type=MESH,
        )

    def state_copy(bit, j):
        return pltpu.make_async_remote_copy(
            src_ref=send_ref.at[bit, j],
            dst_ref=recv_ref.at[bit, j],
            send_sem=send_sem.at[bit, j],
            recv_sem=recv_sem.at[bit, j],
            device_id={"seq": own_seq ^ (1 << bit), "head": own_head},
            device_id_type=MESH,
        )

    def decay_copy(bit):
        return pltpu.make_async_remote_copy(
            src_ref=decay_send_ref.at[bit],
            dst_ref=decay_recv_ref.at[bit],
            send_sem=decay_send_sem.at[bit],
            recv_sem=decay_recv_sem.at[bit],
            device_id={"seq": own_seq ^ (1 << bit), "head": own_head},
            device_id_type=MESH,
        )

    def square_copy(step):
        return pltpu.make_async_remote_copy(
            src_ref=square_send_ref,
            dst_ref=square_recv_ref.at[step - 1],
            send_sem=square_send_sem.at[step - 1],
            recv_sem=square_recv_sem.at[step - 1],
            device_id={"seq": own_seq, "head": lax.rem(own_head + step, head_axis)},
            device_id_type=MESH,
        )

    row_id = lax.broadcasted_iota(jnp.int32, (rows, rows), 0)
    col_id = lax.broadcasted_iota(jnp.int32, (rows, rows), 1)
    order_ref[...] = (row_id <= col_id).astype(F32).astype(BF16)
    whole_row = lax.broadcasted_iota(jnp.int32, (heads, width), 0)
    whole_lane = lax.broadcasted_iota(jnp.int32, (heads, width), 1) // HEADDIM
    whole_spread = (whole_row == whole_lane).astype(F32).astype(BF16)
    lane = lax.broadcasted_iota(jnp.int32, (heads, rows), 1)

    loads[0].wait()
    loads[1].wait()
    log_decay = decay_ref[...]
    high, rest = split(log_decay)
    middle, low = split(log_decay - high.astype(F32))
    total = mm(jnp.concatenate([high, middle, low], axis=0), order_ref[...])
    total = total[0:heads] + (total[heads : 2 * heads] + total[2 * heads : 3 * heads])
    doc_row = lax.broadcasted_iota(jnp.int32, (stretches, rows), 0)
    doc_lane = lax.broadcasted_iota(jnp.int32, (stretches, rows), 1) // STRETCH
    doc_order = (doc_row <= doc_lane).astype(F32).astype(BF16)
    doc = jnp.broadcast_to(doc_ref[...].astype(F32), (16, stretches)).astype(BF16)
    count = mm(doc, doc_order)
    if heads != 16:
        count = jnp.broadcast_to(count[0:1], (heads, rows))

    def at_edges(array, size, edge):
        pieces = []
        for start in range(0, rows, max(size, 128)):
            piece = jnp.broadcast_to(
                array[:, start + edge : start + edge + 1], (heads, max(size, 128))
            )
            if size < 128:
                other = jnp.broadcast_to(
                    array[:, start + size + edge : start + size + edge + 1], (heads, 128)
                )
                piece = jnp.where(lane[:, 0:128] < size, piece, other)
            pieces.append(piece)
        return jnp.concatenate(pieces, axis=1) if len(pieces) > 1 else pieces[0]

    end_log = total[:, rows - 1 : rows]
    end_count = count[:, rows - 1 : rows]
    same_end = (count == end_count).astype(F32)
    loads[2].wait()
    step = step_ref[...]
    end_factor = jnp.exp(end_log - total) * step * same_end
    end_factor_ref[...] = end_factor.T.astype(BF16)

    def widen(column):
        a = jnp.broadcast_to(column, (heads, 128)).T[0:16, :]
        first, rest = split(a)
        second, third = split(rest32(a, first))
        stacked = jnp.concatenate([first, second, third], axis=0)
        whole = mm(stacked, whole_spread)
        return whole[0:1] + (whole[16:17] + whole[32:33])

    def rest32(a, first):
        return a - first.astype(F32)

    span_decay = widen(jnp.exp(end_log) * (end_count == 0.0).astype(F32))
    decay_send_ref[0] = span_decay

    loads[3].wait()
    loads[4].wait()
    for j in range(CHUNKS):
        lanes = slice(j * chunk, (j + 1) * chunk)
        carried = (
            mm(end_factor_ref[...], whole_spread[:, lanes]) * values_ref[:, lanes].astype(F32)
        ).astype(BF16)
        state = tn(key_ref[...], carried)
        block_ref[j] = state
        send_ref[0, j] = state.astype(BF16)
        if j == 0:
            pl.semaphore_wait(barrier, span_bits + head_axis - 1)
            decay_copy(0).start()
        state_copy(0, j).start()

    for load in loads[5:]:
        load.wait()
    picked = (
        lax.broadcasted_iota(jnp.int32, (table_rows, rows), 0) == pick_ref[...]
    )
    picked = picked.astype(F32).astype(BF16)

    def weight(level):
        table_high, table_low = split(table_ref[level])
        return tn(table_high, picked) + tn(table_low, picked)

    factors = []
    offset = total - at_edges(total, STRETCH, STRETCH // 2)
    factors.append(jnp.exp(-offset) * step)
    factors.append(jnp.exp(offset) * weight(0))
    for level in range(1, low_bits + 1):
        size = STRETCH << level
        offset = total - at_edges(total, size, size // 2 - 1)
        keep = (count == at_edges(count, size, size // 2 - 1)).astype(F32)
        after = lane % size >= size // 2
        decayed = jnp.exp(jnp.minimum(jnp.where(after, offset, -offset), 0.0))
        factors.append(decayed * keep * jnp.where(after, weight(level), step))
    reach = jnp.exp(total) * (count == 0.0).astype(F32)
    for bit in range(span_bits):
        upper = lax.rem(own_seq >> bit, 2).astype(F32)
        factors.append(reach * weight(1 + low_bits + bit) * upper)
    per_group = 128 // heads
    for group in range(factor_ref.shape[0]):
        part = factors[group * per_group : (group + 1) * per_group]
        part = part + [jnp.zeros((heads, rows), F32)] * (per_group - len(part))
        factor_ref[group] = jnp.concatenate(part, axis=0).T.astype(BF16)

    spread_row = lax.broadcasted_iota(jnp.int32, (128, chunk), 0)
    spread_lane = lax.broadcasted_iota(jnp.int32, (128, chunk), 1) // HEADDIM

    def spread(k, j):
        first = (k % per_group) * heads + j * (chunk // HEADDIM)
        pick = (spread_row == spread_lane + first).astype(F32).astype(BF16)
        return mm(factor_ref[k // per_group], pick)

    tri_row = lax.broadcasted_iota(jnp.int32, (STRETCH, STRETCH), 0)
    tri_col = lax.broadcasted_iota(jnp.int32, (STRETCH, STRETCH), 1)
    for c in range(stretches):
        here = slice(c * STRETCH, (c + 1) * STRETCH)
        line = nt(query_ref[here, :], key_ref[0 : (c + 1) * STRETCH, :])
        if c:
            score_ref[here, 0 : c * STRETCH] = line[:, 0 : c * STRETCH].astype(BF16)
        score_ref[here, here] = jnp.where(tri_row >= tri_col, line[:, here], 0.0).astype(BF16)

    skip_high, skip_rest = split(jnp.broadcast_to(skip_ref[...], (16, heads)))
    skip_low = (skip_ref[...] - skip_high[0:1].astype(F32)).astype(BF16)
    skip = mm(skip_high, whole_spread) + mm(jnp.broadcast_to(skip_low, (16, heads)), whole_spread)
    skip = skip[0:1, :]

    def local_part(j):
        lanes = slice(j * chunk, (j + 1) * chunk)
        values = values_ref[:, lanes].astype(F32)
        weighted_ref[...] = (spread(0, j) * values).astype(BF16)
        scale = spread(1, j)
        base = skip[:, lanes] * values
        for c in range(stretches):
            here = slice(c * STRETCH, (c + 1) * STRETCH)
            sum_ref[j, here, :] = base[here, :] + scale[here, :] * mm(
                score_ref[here, here], weighted_ref[here, :]
            )
        for level in range(1, low_bits + 1):
            half = STRETCH << (level - 1)
            scale = spread(1 + level, j)
            for start in range(0, rows, 2 * half):
                before = slice(start, start + half)
                after = slice(start + half, start + 2 * half)
                weighted = (scale[before, :] * values[before, :]).astype(BF16)
                sum_ref[j, after, :] += scale[after, :] * mm(score_ref[after, before], weighted)

    def gate_part(j):
        gate = gate_ref[:, j * chunk : (j + 1) * chunk].astype(F32)
        gate_act_ref[j] = gate * (0.5 + 0.5 * jnp.tanh(0.5 * gate))

    def add_remote(bit, j):
        sum_ref[j] += spread(2 + low_bits + bit, j) * mm(query_ref[...], remote_ref[bit, j])

    own_half = lax.rem(own_seq, 2)
    last = span_bits - 1

    def forward_copy(bit, i):
        j = 2 * i + own_half
        return pltpu.make_async_remote_copy(
            src_ref=recv_ref.at[bit, j],
            dst_ref=recv_ref.at[bit, j],
            send_sem=forward_sem.at[bit, i],
            recv_sem=recv_sem.at[bit, j],
            device_id={"seq": own_seq ^ 1, "head": own_head},
            device_id_type=MESH,
        )

    def merge(bit, j):
        other = recv_ref[bit, j].astype(F32)
        if bit < last:
            merged = row_ref[0, j] * block_ref[j] + row_ref[1, j] * other
            block_ref[j] = merged
            send_ref[bit + 1, j] = merged.astype(BF16)
        return other

    def finish(j):
        gated = sum_ref[j] * gate_act_ref[j]
        sum_ref[j] = gated
        square_ref[...] += gated * gated

    square_ref[...] = jnp.zeros_like(square_ref)
    block_decay = span_decay
    lead_decay = jnp.ones_like(span_decay)
    for bit in range(span_bits):
        upper = lax.rem(own_seq >> bit, 2).astype(F32)
        decay_copy(bit).wait()
        other_decay = decay_recv_ref[bit]
        keep_own = upper + (1.0 - upper) * other_decay
        keep_other = upper * block_decay + (1.0 - upper)
        next_decay = block_decay * other_decay
        if bit < last:
            decay_send_ref[bit + 1] = next_decay
            decay_copy(bit + 1).start()
        for j in range(CHUNKS):
            lanes = slice(j * chunk, (j + 1) * chunk)
            row_ref[0, j] = keep_own[:, lanes]
            row_ref[1, j] = keep_other[:, lanes]
            row_ref[2, j] = lead_decay[:, lanes]
        if bit < 2:
            for j in range(CHUNKS):
                state_copy(bit, j).wait()
                other = merge(bit, j)
                if bit + 1 < min(2, span_bits):
                    state_copy(bit + 1, j).start()
                elif bit < last:

                    @pl.when(own_half == j % 2)
                    def _():
                        state_copy(bit + 1, j).start()

                remote_ref[bit, j] = (row_ref[2, j] * other).astype(BF16)
                if bit == 0:
                    local_part(j)
                else:
                    add_remote(0, j)
            if bit == last:
                for j in range(CHUNKS):
                    add_remote(last, j)
                    gate_part(j)
            elif bit == 1:
                for j in range(CHUNKS // 2):
                    gate_part(j)
        else:
            for i in range(CHUNKS // 2):
                j = 2 * i + own_half
                state_copy(bit, j).wait()
                forward_copy(bit, i).start()
                if bit == 2:
                    add_remote(1, 2 * i)
                    add_remote(1, 2 * i + 1)
                    gate_part(CHUNKS // 2 + i)
            for i in range(CHUNKS // 2):
                j = 2 * i + own_half
                other = merge(bit, j)
                if bit < last:
                    state_copy(bit + 1, j).start()
                remote_ref[bit, j] = (row_ref[2, j] * other).astype(BF16)
                add_remote(bit, j)
                if bit == last:
                    finish(j)
            for i in range(CHUNKS // 2):
                j = 2 * i + 1 - own_half
                state_copy(bit, j).wait_recv()
                other = merge(bit, j)
                remote_ref[bit, j] = (row_ref[2, j] * other).astype(BF16)
                add_remote(bit, j)
                if bit == last:
                    finish(j)
            for i in range(CHUNKS // 2):
                forward_copy(bit, i).wait_send()
        lead_decay = lead_decay * (upper * other_decay + (1.0 - upper))
        block_decay = next_decay
    if span_bits == 0:
        for j in range(CHUNKS):
            local_part(j)
            gate_part(j)
    if span_bits < 3:
        for j in range(CHUNKS):
            finish(j)

    squares = square_ref[...]
    ones = jnp.ones((16, chunk), BF16)
    square_high, square_low = split(squares)
    square_row = nt(ones, square_high) + nt(ones, square_low)
    square_send_ref[...] = square_row[0:1, :]
    for step in range(1, head_axis):
        square_copy(step).start()
    square_total = square_row[0:1, :]
    for step in range(1, head_axis):
        square_copy(step).wait()
        square_total = square_total + square_recv_ref[step - 1]
    mean_square = square_total * (1.0 / (width * head_axis))
    inverse = lax.rsqrt(mean_square + epsilon)
    inverse = jnp.broadcast_to(inverse, (8, rows)).T[:, 0:1]
    for j in range(CHUNKS):
        lanes = slice(j * chunk, (j + 1) * chunk)
        out_ref[:, lanes] = (sum_ref[j] * inverse * gain_ref[:, lanes]).astype(BF16)


def local(
    span_bits,
    head_axis,
    values_in,
    gate_in,
    key_proj,
    query_proj,
    step_size,
    log_decay,
    skip_weight,
    norm_gain,
    level_table,
    level_pick,
    doc_start,
):
    rows, width = values_in.shape
    heads = step_size.shape[1]
    states = key_proj.shape[1]
    low_bits = (rows // STRETCH).bit_length() - 1
    chunk = width // CHUNKS
    hbm = pl.BlockSpec(memory_space=pltpu.HBM)
    bits = max(span_bits, 1)
    peers = max(head_axis - 1, 1)
    factor_count = 2 + low_bits + span_bits
    groups = -(-factor_count // (128 // heads))
    operands = (
        values_in,
        gate_in,
        key_proj,
        query_proj,
        step_size.T,
        log_decay.T,
        skip_weight.reshape(1, heads),
        norm_gain.reshape(1, width),
        level_table.transpose(2, 0, 1),
        level_pick.reshape(1, rows),
        doc_start.reshape(1, rows // STRETCH),
    )
    return pl.pallas_call(
        functools.partial(kernel, span_bits, head_axis),
        out_shape=jax.ShapeDtypeStruct((rows, width), BF16),
        in_specs=[hbm] * len(operands),
        out_specs=pl.BlockSpec(memory_space=pltpu.VMEM),
        scratch_shapes=[pltpu.VMEM(a.shape, a.dtype) for a in operands]
        + [
            pltpu.VMEM((rows, rows), BF16),
            pltpu.VMEM((rows, heads), BF16),
            pltpu.VMEM((groups, rows, 128), BF16),
            pltpu.VMEM((rows, rows), BF16),
            pltpu.VMEM((rows, chunk), BF16),
            pltpu.VMEM((CHUNKS, rows, chunk), F32),
            pltpu.VMEM((CHUNKS, rows, chunk), F32),
            pltpu.VMEM((CHUNKS, states, chunk), F32),
            pltpu.VMEM((bits, CHUNKS, states, chunk), BF16),
            pltpu.VMEM((bits, CHUNKS, states, chunk), BF16),
            pltpu.VMEM((bits, CHUNKS, states, chunk), BF16),
            pltpu.VMEM((bits, 1, width), F32),
            pltpu.VMEM((bits, 1, width), F32),
            pltpu.VMEM((1, rows), F32),
            pltpu.VMEM((peers, 1, rows), F32),
            pltpu.VMEM((3, CHUNKS, 1, chunk), F32),
            pltpu.VMEM((rows, chunk), F32),
            pltpu.SemaphoreType.DMA((len(operands),)),
            pltpu.SemaphoreType.DMA((bits, CHUNKS)),
            pltpu.SemaphoreType.DMA((bits, CHUNKS)),
            pltpu.SemaphoreType.DMA((bits,)),
            pltpu.SemaphoreType.DMA((bits,)),
            pltpu.SemaphoreType.DMA((peers,)),
            pltpu.SemaphoreType.DMA((peers,)),
            pltpu.SemaphoreType.DMA((bits, CHUNKS)),
        ],
        compiler_params=pltpu.CompilerParams(
            collective_id=0, has_side_effects=True, vmem_limit_bytes=60 * 1024 * 1024
        ),
    )(*operands)


def solution(mesh):
    in_specs = (
        P("seq", "head"),
        P("seq", "head"),
        P("seq", None),
        P("seq", None),
        P("seq", "head"),
        P("seq", "head"),
        P("head"),
        P("head"),
        P(None, "head", None),
        P("seq"),
        P("seq"),
    )
    span_bits = mesh.shape["seq"].bit_length() - 1
    body = functools.partial(local, span_bits, mesh.shape["head"])
    return jax.shard_map(
        body, mesh=mesh, in_specs=in_specs, out_specs=P("seq", "head"), check_vma=False
    )
```
